32 devices in a mesh: grp: 2 (over x), pq: 16 (over z, y, core).
Axes of the slice: x: 2, y: 2, z: 4, core: 2. Of those that a mesh axis runs over, the one named last changes fastest.
Arguments:
- pair_blocks: bfloat16 [4, 288, 128, 128], P('grp', 'pq'), may hold values from -6 to 6
- block_list: int32 [4, 288], P('grp', 'pq'), may hold values from 0 to 2047, as said below
- block_count: int32 [4, 16], P('grp', 'pq'), may hold values from 1 to 18, as said below
- coef: bfloat16 [4096, 512], P('pq', 'grp'), may hold values from -0.09375 to 0.09375
Outputs:
- transformed: float32 [8, 512, 512], P('grp', 'pq')
The draws below stay inside these ranges and needn't reach their ends.
Inputs may be any that keep to these rules, and one draw needn't show every extreme that they name: `block_list`: within one row the ids are distinct, each in 0 to 2 * 32^2 - 1. `block_count`: in every row some device has exactly 18 live slots.
All inputs are finite; a program needn't handle non-finite values.
Results may differ from the reference program's by a relative error of at most 0.0042.
Values may be sent and summed in bfloat16 or wider, within the bound.
A program may use at most 64 MiB of HBM per device.

```python
import jax
import jax.numpy as jnp
from jax import lax

NAO = 4096
NMO = 512
TILE = 128
KL_PANEL = 2
PANELS = 2
SLOTS = 18
NKL = 8
N_GRP = 2
N_PQ = 16


def draw_block_list(key, part):
    total_rows = PANELS * N_GRP
    keys = jax.random.split(jax.random.fold_in(key, 11), total_rows)
    idents = KL_PANEL * (NAO // TILE) * (NAO // TILE)

    def one_row(row_key):
        return jax.random.permutation(row_key, idents)[:N_PQ * SLOTS]
    return jax.vmap(one_row)(keys).astype(jnp.int32)


def draw_block_count(key, part):
    total_rows = PANELS * N_GRP
    first_key, second_key, third_key = jax.random.split(jax.random.fold_in(key, 23), 3)
    low = max(SLOTS // 2, 1)
    high = max(SLOTS, low + 1)
    first = jax.random.randint(first_key, (total_rows, N_PQ), low, high)
    second = jax.random.randint(second_key, (total_rows, N_PQ), low, high)
    counts = 1 + first * second // SLOTS
    counts = jnp.minimum(counts, SLOTS)
    busiest = jax.random.randint(third_key, (total_rows, 1), 0, N_PQ)
    places = jnp.arange(N_PQ, dtype=jnp.int32)[None, :]
    counts = jnp.where(places == busiest, SLOTS, counts)
    return counts.astype(jnp.int32)


def shard_levels(stream_key, shape, cuts, smallest, high):
    loudness, own = 1.0, jax.random.fold_in(stream_key, 6)
    for position, shards_of in cuts:
        steps = jnp.exp(jax.random.uniform(jax.random.fold_in(own, position), (shards_of,), jnp.float32, smallest / len(cuts), high / len(cuts)))
        loudness = loudness * jnp.repeat(steps, shape[position] // shards_of).reshape([-1 if axis == position else 1 for axis in range(len(shape))])
    return loudness


def scatter_about(stream_key, shape, width, most, cuts=(), kind=jnp.bfloat16):
    factor_of = shard_levels(stream_key, shape, cuts, -0.22, 0.18) if cuts else 1.0
    entries = jax.random.normal(stream_key, shape, jnp.float32) * width * factor_of
    return jnp.minimum(jnp.maximum(entries, -most), most).astype(kind)


def setup_inputs(seed: int = 0) -> dict:
    key_list = jax.random.split(jax.random.key(seed), 5)
    return {
        "pair_blocks": scatter_about(key_list[0], (PANELS * N_GRP, N_PQ * SLOTS, TILE, TILE), 1.0, 6.0, ((0, 2), (1, 16))),
        "block_list": draw_block_list(jax.random.fold_in(key_list[4], 71), 0),
        "block_count": draw_block_count(jax.random.fold_in(key_list[4], 71), 0),
        "coef": scatter_about(key_list[3], (NAO, NMO), NAO ** -0.5, 0.09375, ((0, 16), (1, 2))),
    }


def reference(pair_blocks, block_list, block_count, coef):
    nblk = NAO // TILE
    per_kl = nblk * nblk

    def one_row(inputs):
        blocks, idents, counts = inputs

        def step(acc, slot):
            live = (slot % SLOTS) < counts[slot // SLOTS]

            def add(total):
                ident = idents[slot]
                which = (ident // per_kl).astype(jnp.int32)
                row_blk = ((ident // nblk) % nblk).astype(jnp.int32)
                col_blk = (ident % nblk).astype(jnp.int32)
                col_coef = lax.dynamic_slice_in_dim(coef, col_blk * TILE, TILE, 0)
                row_coef = lax.dynamic_slice_in_dim(coef, row_blk * TILE, TILE, 0)
                block = lax.dynamic_index_in_dim(blocks, slot, 0, keepdims=False)
                half = jnp.dot(block, col_coef, preferred_element_type=jnp.float32).astype(jnp.bfloat16)
                term = jnp.dot(row_coef.T, half, preferred_element_type=jnp.float32)
                current = lax.dynamic_index_in_dim(total, which, 0, keepdims=False)
                return lax.dynamic_update_index_in_dim(total, current + term, which, 0)

            return lax.cond(live, add, lambda total: total, acc), None

        start = jnp.zeros((KL_PANEL, NMO, NMO), jnp.float32)
        result, _ = lax.scan(step, start, jnp.arange(N_PQ * SLOTS, dtype=jnp.int32))
        return result

    rows = lax.map(one_row, (pair_blocks, block_list, block_count))
    return rows.reshape(NKL, NMO, NMO)
```

```python
import functools

import jax
import jax.numpy as jnp
from jax import lax
from jax.experimental import pallas as pl
from jax.experimental.pallas import tpu as pltpu
from jax.sharding import PartitionSpec as P

KL_PANEL = 2
MESH = pl.DeviceIdType.MESH
DIRECT_LIMIT = 64
UNROLL = 3


def coords(mine, n_z):
    core, yy, zz = lax.rem(mine, 2), lax.rem(lax.div(mine, 2), 2), lax.div(mine, 4)
    return core, yy, zz, lambda step: lax.rem(zz + step, n_z)


def pq_of(z, y, c):
    return z * 4 + y * 2 + c


def meet(peers):
    barrier = pltpu.get_barrier_semaphore()
    for peer in peers:
        pl.semaphore_signal(barrier, inc=1, device_id=peer, device_id_type=MESH)
    pl.semaphore_wait(barrier, len(peers))


def gather_kernel(n_grp, n_pq, tile, coef_ref, full, flipped, send_sem, recv_sem):
    rows, cols = coef_ref.shape
    n_z = n_pq // 4
    mine_g, mine = lax.axis_index("grp"), lax.axis_index("pq")
    core, yy, zz, z_at = coords(mine, n_z)
    core_peer = (mine_g, pq_of(zz, yy, 1 - core))
    y_peer = (mine_g, pq_of(zz, 1 - yy, core))
    x_peer = (1 - mine_g, mine)
    z_peers = [(mine_g, pq_of(z_at(s), yy, core)) for s in range(1, n_z)]
    meet([core_peer, y_peer, x_peer] + z_peers)

    first_g = lax.rem(mine_g + 1 - core, 2)
    first_y = lax.rem(yy + core, 2)
    second_g = lax.rem(mine_g + core, 2)
    second_y = lax.rem(yy + 1 - core, 2)
    first_peer = (first_g, pq_of(zz, first_y, core))
    second_peer = (second_g, pq_of(zz, second_y, core))
    started = []

    def place(g, p):
        return full.at[g, pl.ds(pl.multiple_of(p * rows, rows), rows), :]

    def send(src, g, p, peer):
        copy = pltpu.make_async_remote_copy(
            src_ref=src, dst_ref=place(g, p), send_sem=send_sem.at[len(started)],
            recv_sem=recv_sem.at[g, p], device_id=peer, device_id_type=MESH,
        )
        copy.start()
        started.append(copy)

    def flip(src, g, p):
        turned = src[...].T
        for k in range(rows // tile):
            flipped[p * (rows // tile) + k, pl.ds(pl.multiple_of(g * cols, cols), cols), :] = (
                turned[:, k * tile:(k + 1) * tile]
            )

    def relay(g, p, targets):
        pltpu.make_async_copy(place(g, p), place(g, p), recv_sem.at[g, p]).wait()
        for peer in targets:
            send(place(g, p), g, p, peer)
        flip(place(g, p), g, p)

    for peer in [first_peer, second_peer] + z_peers + [core_peer]:
        send(coef_ref, mine_g, mine, peer)
    full[mine_g, pl.ds(pl.multiple_of(mine * rows, rows), rows), :] = coef_ref[...]
    flip(coef_ref, mine_g, mine)
    order = [1, n_z - 1] + list(range(2, n_z - 1))
    relay(first_g, pq_of(zz, first_y, core), [second_peer, core_peer])
    for step in order:
        relay(mine_g, pq_of(z_at(step), yy, core), [first_peer, second_peer, core_peer])
    for step in order:
        relay(first_g, pq_of(z_at(step), first_y, core), [second_peer, core_peer])
    for step in [0] + order:
        relay(second_g, pq_of(z_at(step), second_y, core), [core_peer])
    for step in [0] + order:
        relay(1 - mine_g, pq_of(z_at(step), 1 - yy, core), [core_peer])
    for g, y in ((mine_g, yy), (1 - mine_g, yy), (mine_g, 1 - yy), (1 - mine_g, 1 - yy)):
        for step in [0] + order:
            relay(g, pq_of(z_at(step), y, 1 - core), [])
    for copy in started:
        copy.wait_send()


def transform_kernel(
    n_grp, n_pq, blocks_ref, list_ref, count_ref, full, flipped,
    own_ref, other_ref, rows_p, halves, acc,
):
    panels, slots, tile = blocks_ref.shape[0], blocks_ref.shape[1], blocks_ref.shape[2]
    nblk, width = flipped.shape[0], flipped.shape[1]
    cols, chunk, n_z = width // n_grp, width // n_pq, n_pq // 4
    core = lax.rem(lax.axis_index("pq"), 2)
    pair = 2 * tile

    for panel in range(panels):
        count = count_ref[panel, 0]

        def step(turn, used):
            for k in range(UNROLL):
                slot = turn * UNROLL + k
                live = slot < count
                slot = jnp.minimum(slot, slots - 1)
                ident = list_ref[panel, slot]
                which = jnp.where(live, lax.div(ident, nblk * nblk), KL_PANEL)
                row_blk = lax.rem(lax.div(ident, nblk), nblk)
                col_blk = lax.rem(ident, nblk)
                spot = jnp.where(which == 0, used[0], jnp.where(which == 1, used[1], 0))
                used = tuple(u + jnp.where(which == kl, 1, 0) for kl, u in enumerate(used))
                at = pl.ds(pl.multiple_of(spot * tile, tile), tile)
                rows_p[which, :, at] = flipped[row_blk]
                for g in range(n_grp):
                    coefs = full[g, pl.ds(pl.multiple_of(col_blk * tile, tile), tile), :]
                    half = jnp.dot(blocks_ref[panel, slot], coefs, preferred_element_type=jnp.float32)
                    halves[which, at, g * cols:(g + 1) * cols] = half.astype(jnp.bfloat16)
            return used

        zero = jnp.int32(0)
        used = lax.fori_loop(0, lax.div(count + UNROLL - 1, UNROLL), step, (zero,) * KL_PANEL)
        for kl in range(KL_PANEL):
            at = pl.ds(pl.multiple_of(used[kl] * tile, tile), tile)
            rows_p[kl, :, at] = jnp.zeros((width, tile), jnp.bfloat16)
            halves[kl, at, :] = jnp.zeros((tile, width), jnp.bfloat16)
            acc[...] = jnp.zeros_like(acc)

            def add(turn, carry):
                at = pl.ds(pl.multiple_of(turn * pair, pair), pair)
                acc[...] += jnp.dot(
                    rows_p[kl, :, at], halves[kl, at, :], preferred_element_type=jnp.float32
                )
                return carry

            lax.fori_loop(0, lax.div(used[kl] + 1, 2), add, 0)
            for y in range(2):
                for z in range(n_z):
                    for c, ref in ((core, own_ref), (1 - core, other_ref)):
                        at = pl.multiple_of((z * 4 + y * 2 + c) * chunk, chunk)
                        ref[panel, y, z, kl] = acc[pl.ds(at, chunk), :].astype(ref.dtype)


def scatter_kernel(
    own, other, out_ref, sum_bf, fin_bf, from_core, from_y, from_z,
    send_sem, core_recv, y_recv, z_recv,
):
    panels, n_z = own.shape[0], own.shape[2]
    f32, bf16 = jnp.float32, jnp.bfloat16
    mine_g, mine = lax.axis_index("grp"), lax.axis_index("pq")
    core, yy, zz, z_at = coords(mine, n_z)
    core_peer = (mine_g, pq_of(zz, yy, 1 - core))
    y_peer = (mine_g, pq_of(zz, 1 - yy, core))
    z_peers = [(mine_g, pq_of(z_at(s), yy, core)) for s in range(1, n_z)]
    meet([core_peer, y_peer] + z_peers)
    sent = []

    def push(src, dst, recv, peer):
        copy = pltpu.make_async_remote_copy(
            src_ref=src, dst_ref=dst, send_sem=send_sem.at[len(sent)],
            recv_sem=recv, device_id=peer, device_id_type=MESH,
        )
        copy.start()
        sent.append(copy)

    def landed(dst, recv):
        pltpu.make_async_copy(dst, dst, recv).wait()

    far_first = list(range(1, n_z)) + [0]
    for y in (1 - yy, yy):
        for panel in range(panels):
            push(other.at[panel, y], from_core.at[panel, y], core_recv.at[panel, y], core_peer)
    for panel in range(panels):
        landed(from_core.at[panel, 1 - yy], core_recv.at[panel, 1 - yy])
    for s in far_first:
        z = z_at(s)
        for panel in range(panels):
            total = own[panel, 1 - yy, z] + from_core[panel, 1 - yy, z].astype(f32)
            sum_bf[panel, s] = total.astype(bf16)
            push(sum_bf.at[panel, s], from_y.at[panel, s], y_recv.at[panel, s], y_peer)
    for panel in range(panels):
        landed(from_core.at[panel, yy], core_recv.at[panel, yy])
    for s in far_first:
        z = z_at(s)
        for panel in range(panels):
            landed(from_y.at[panel, s], y_recv.at[panel, s])
            total = (
                own[panel, yy, z] + from_core[panel, yy, z].astype(f32)
                + from_y[panel, s].astype(f32)
            )
            if s:
                fin_bf[panel, s] = total.astype(bf16)
                push(fin_bf.at[panel, s], from_z.at[panel, s], z_recv.at[panel, s], z_peers[s - 1])
            else:
                out_ref[pl.ds(panel * KL_PANEL, KL_PANEL)] = total
    for panel in range(panels):
        total = out_ref[pl.ds(panel * KL_PANEL, KL_PANEL)]
        for s in range(1, n_z):
            landed(from_z.at[panel, s], z_recv.at[panel, s])
            total += from_z[panel, s].astype(f32)
        out_ref[pl.ds(panel * KL_PANEL, KL_PANEL)] = total
    for copy in sent:
        copy.wait_send()


def direct(n_grp, n_pq, pair_blocks, block_list, block_count, coef):
    panels, slots, tile, _ = pair_blocks.shape
    rows, cols = coef.shape
    width, nao, n_z = n_grp * cols, n_pq * rows, n_pq // 4
    chunk = width // n_pq
    bf16, f32 = jnp.bfloat16, jnp.float32
    vmem = pl.BlockSpec(memory_space=pltpu.VMEM)
    smem = pl.BlockSpec(memory_space=pltpu.SMEM)
    sems = pltpu.SemaphoreType.DMA
    shape = jax.ShapeDtypeStruct
    mib = 2**20
    n_gather = 2 + n_z + 3 * (n_z - 1) + 2 * n_z + 2 * n_z
    full, flipped = pl.pallas_call(
        functools.partial(gather_kernel, n_grp, n_pq, tile),
        out_shape=(shape((n_grp, nao, cols), bf16), shape((nao // tile, width, tile), bf16)),
        in_specs=[vmem],
        out_specs=(vmem, vmem),
        scratch_shapes=[sems((n_gather,)), sems((n_grp, n_pq))],
        compiler_params=pltpu.CompilerParams(
            collective_id=0, has_side_effects=True, vmem_limit_bytes=24 * mib
        ),
    )(coef)
    padded = slots + 1 + slots % 2
    part = (panels, 2, n_z, KL_PANEL, chunk, width)
    own, other = pl.pallas_call(
        functools.partial(transform_kernel, n_grp, n_pq),
        out_shape=(shape(part, f32), shape(part, bf16)),
        in_specs=[vmem, smem, smem, vmem, vmem],
        out_specs=(vmem, vmem),
        scratch_shapes=[
            pltpu.VMEM((KL_PANEL + 1, width, padded * tile), bf16),
            pltpu.VMEM((KL_PANEL + 1, padded * tile, width), bf16),
            pltpu.VMEM((width, width), f32),
        ],
        compiler_params=pltpu.CompilerParams(vmem_limit_bytes=40 * mib),
    )(pair_blocks, block_list, block_count, full, flipped)
    pieces = (panels, n_z, KL_PANEL, chunk, width)
    return pl.pallas_call(
        scatter_kernel,
        out_shape=shape((panels * KL_PANEL, chunk, width), f32),
        in_specs=[vmem, vmem],
        out_specs=vmem,
        scratch_shapes=[
            pltpu.VMEM(pieces, bf16),
            pltpu.VMEM(pieces, bf16),
            pltpu.VMEM(part, bf16),
            pltpu.VMEM(pieces, bf16),
            pltpu.VMEM(pieces, bf16),
            sems((panels * (1 + 2 * n_z) + panels,)),
            sems((panels, 2)),
            sems((panels, n_z)),
            sems((panels, n_z)),
        ],
        compiler_params=pltpu.CompilerParams(
            collective_id=1, has_side_effects=True, vmem_limit_bytes=24 * mib
        ),
    )(own, other)


def local_kernel(nblk, blocks_ref, list_ref, count_ref, coef_ref, out_ref):
    panels, slots, tile = blocks_ref.shape[0], blocks_ref.shape[1], blocks_ref.shape[2]
    out_ref[...] = jnp.zeros_like(out_ref)
    for panel in range(panels):

        def step(slot, carry):
            ident = list_ref[panel, slot]
            which = panel * KL_PANEL + lax.div(ident, nblk * nblk)
            row_blk = lax.rem(lax.div(ident, nblk), nblk)
            col_blk = lax.rem(ident, nblk)
            col_coef = coef_ref[pl.ds(pl.multiple_of(col_blk * tile, tile), tile), :]
            row_coef = coef_ref[pl.ds(pl.multiple_of(row_blk * tile, tile), tile), :]
            half = jnp.dot(blocks_ref[panel, slot], col_coef, preferred_element_type=jnp.float32)
            out_ref[which] += lax.dot_general(
                row_coef, half.astype(jnp.bfloat16), (((0,), (0,)), ((), ())),
                preferred_element_type=jnp.float32,
            )
            return carry

        lax.fori_loop(0, count_ref[panel, 0], step, 0)


def gathered(pair_blocks, block_list, block_count, coef):
    coef_rows = lax.all_gather(coef, "pq", axis=0, tiled=True)
    coef_full = lax.all_gather(coef_rows, "grp", axis=1, tiled=True)
    nao, width = coef_full.shape
    vmem = pl.BlockSpec(memory_space=pltpu.VMEM)
    smem = pl.BlockSpec(memory_space=pltpu.SMEM)
    joined = pl.pallas_call(
        functools.partial(local_kernel, nao // pair_blocks.shape[2]),
        out_shape=jax.ShapeDtypeStruct((pair_blocks.shape[0] * KL_PANEL, width, width), jnp.float32),
        in_specs=[vmem, smem, smem, vmem],
        out_specs=vmem,
        compiler_params=pltpu.CompilerParams(vmem_limit_bytes=48 * 2**20),
    )(pair_blocks, block_list, block_count, coef_full)
    return lax.psum_scatter(joined, "pq", scatter_dimension=1, tiled=True)


def body(pair_blocks, block_list, block_count, coef):
    n_grp, n_pq = lax.axis_size("grp"), lax.axis_size("pq")
    rows, cols = coef.shape
    tile = pair_blocks.shape[2]
    fits = n_grp == 2 and n_pq % 8 == 0 and n_grp * n_pq <= DIRECT_LIMIT
    if fits and rows % tile == 0 and cols % 128 == 0:
        return direct(n_grp, n_pq, pair_blocks, block_list, block_count, coef)
    return gathered(pair_blocks, block_list, block_count, coef)


def solution(mesh):
    in_specs = (P("grp", "pq", None, None), P("grp", "pq"), P("grp", "pq"), P("pq", "grp"))
    out_specs = P("grp", "pq", None)
    return jax.shard_map(body, mesh=mesh, in_specs=in_specs, out_specs=out_specs, check_vma=False)
```

```python
import functools

import jax
import jax.numpy as jnp
from jax import lax
from jax.experimental import pallas as pl
from jax.experimental.pallas import tpu as pltpu
from jax.sharding import PartitionSpec as P

KL_PANEL = 2
MESH = pl.DeviceIdType.MESH
UNROLL = 3


LINE = 4


def coords(mine):
    core, yy, zz = lax.rem(mine, 2), lax.rem(lax.div(mine, 2), 2), lax.div(mine, 4)
    half = lax.div(zz, 2)
    beside = 2 * half + 1 - lax.rem(zz, 2)
    across = 3 - zz
    return core, yy, zz, (beside, 2 - half, 3 - 3 * half), across


def pq_of(z, y, c):
    return z * 4 + y * 2 + c


def meet(peers):
    barrier = pltpu.get_barrier_semaphore()
    for peer in peers:
        pl.semaphore_signal(barrier, inc=1, device_id=peer, device_id_type=MESH)
    pl.semaphore_wait(barrier, len(peers))


def gather_kernel(n_grp, n_pq, tile, coef_ref, full, flipped, send_sem, recv_sem, load_sem):
    rows, cols = coef_ref.shape
    subs = rows // tile
    mine_g, mine = lax.axis_index("grp"), lax.axis_index("pq")
    core, yy, zz, nearest, across = coords(mine)
    middle = (zz > 0) & (zz < LINE - 1)
    core_peer = (mine_g, pq_of(zz, yy, 1 - core))
    y_peer = (mine_g, pq_of(zz, 1 - yy, core))
    x_peer = (1 - mine_g, mine)
    beside_peer = (mine_g, pq_of(nearest[0], yy, core))
    across_peer = (mine_g, pq_of(across, yy, core))

    def place(g, p, k):
        at = pl.multiple_of(p * rows + k * tile, tile)
        return full.at[g, pl.ds(at, tile), :]

    own_rows = full.at[mine_g, pl.ds(pl.multiple_of(mine * rows, rows), rows), :]
    load = pltpu.make_async_copy(coef_ref, own_rows, load_sem)
    load.start()
    meet([core_peer, y_peer, x_peer, beside_peer, across_peer])
    load.wait()

    first_g, first_y = lax.rem(mine_g + 1 - core, 2), lax.rem(yy + core, 2)
    second_g, second_y = lax.rem(mine_g + core, 2), lax.rem(yy + 1 - core, 2)
    first_peer = (first_g, pq_of(zz, first_y, core))
    second_peer = (second_g, pq_of(zz, second_y, core))
    started = []

    def send(g, p, k, peer, only=None):
        copy = pltpu.make_async_remote_copy(
            src_ref=place(g, p, k), dst_ref=place(g, p, k), send_sem=send_sem.at[len(started)],
            recv_sem=recv_sem.at[g, p, k], device_id=peer, device_id_type=MESH,
        )
        if only is None:
            copy.start()
        else:
            pl.when(only)(copy.start)
        started.append((copy, only))

    def flip(g, p, k):
        at = pl.multiple_of(g * cols, cols)
        flipped[p * subs + k, pl.ds(at, cols), :] = place(g, p, k)[...].T

    def await_piece(g, p, k):
        pltpu.make_async_copy(place(g, p, k), place(g, p, k), recv_sem.at[g, p, k]).wait()

    z_of = (zz,) + nearest
    home = {
        "Z": (mine_g, yy), "F": (first_g, first_y),
        "S": (second_g, second_y), "D": (1 - mine_g, 1 - yy),
    }
    twin = {"Z": "Z", "F": "S", "S": "F", "D": "D"}

    def relay(kind, step):
        g, y = home[kind]
        p = pq_of(z_of[step], y, core)
        for k in range(subs):
            await_piece(g, p, k)
            if kind == "Z":
                send(g, p, k, across_peer if step == 1 else beside_peer, middle)
                send(g, p, k, first_peer)
            if kind in "ZF":
                send(g, p, k, second_peer)
            send(g, p, k, core_peer)
            flip(g, p, k)

    def take(kind, step):
        g, y = home[twin[kind]]
        p = pq_of(z_of[step], y, 1 - core)
        for k in range(subs):
            await_piece(g, p, k)
            flip(g, p, k)

    for k in range(subs):
        send(mine_g, mine, k, beside_peer)
        send(mine_g, mine, k, across_peer, middle)
        send(mine_g, mine, k, first_peer)
        send(mine_g, mine, k, second_peer)
    for k in range(subs):
        send(mine_g, mine, k, core_peer)
    for k in range(subs):
        flip(mine_g, mine, k)
    waves = ("Z1 F0", "S0 Z2 F1", "S1 D0 Z3 F2", "S2 D1 F3", "S3 D2 D3")
    before = "Z0"
    for wave in waves:
        for item in wave.split():
            relay(item[0], int(item[1]))
        for item in before.split():
            take(item[0], int(item[1]))
        before = wave
    for item in before.split():
        take(item[0], int(item[1]))
    for copy, only in started:
        if only is None:
            copy.wait_send()
        else:
            pl.when(only)(copy.wait_send)


def transform_kernel(
    n_grp, n_pq, blocks_ref, list_ref, count_ref, full, flipped,
    own_ref, other_ref, rows_p, halves, acc,
):
    panels, slots, tile = blocks_ref.shape[0], blocks_ref.shape[1], blocks_ref.shape[2]
    nblk, width = flipped.shape[0], flipped.shape[1]
    cols, chunk, n_z = width // n_grp, width // n_pq, n_pq // 4
    core = lax.rem(lax.axis_index("pq"), 2)
    pair = 2 * tile

    for panel in range(panels):
        count = count_ref[panel]

        def step(turn, used):
            for k in range(UNROLL):
                slot = turn * UNROLL + k
                live = slot < count
                slot = jnp.minimum(slot, slots - 1)
                ident = list_ref[panel, slot]
                which = jnp.where(live, lax.div(ident, nblk * nblk), KL_PANEL)
                row_blk = lax.rem(lax.div(ident, nblk), nblk)
                col_blk = lax.rem(ident, nblk)
                spot = jnp.where(which == 0, used[0], jnp.where(which == 1, used[1], 0))
                used = tuple(u + jnp.where(which == kl, 1, 0) for kl, u in enumerate(used))
                at = pl.ds(pl.multiple_of(spot * tile, tile), tile)
                rows_p[which, :, at] = flipped[row_blk]
                for g in range(n_grp):
                    coefs = full[g, pl.ds(pl.multiple_of(col_blk * tile, tile), tile), :]
                    half = jnp.dot(blocks_ref[panel, slot], coefs, preferred_element_type=jnp.float32)
                    halves[which, at, g * cols:(g + 1) * cols] = half.astype(jnp.bfloat16)
            return used

        zero = jnp.int32(0)
        used = lax.fori_loop(0, lax.div(count + UNROLL - 1, UNROLL), step, (zero,) * KL_PANEL)
        for kl in range(KL_PANEL):
            at = pl.ds(pl.multiple_of(used[kl] * tile, tile), tile)
            rows_p[kl, :, at] = jnp.zeros((width, tile), jnp.bfloat16)
            halves[kl, at, :] = jnp.zeros((tile, width), jnp.bfloat16)
            acc[...] = jnp.zeros_like(acc)

            def add(turn, carry):
                at = pl.ds(pl.multiple_of(turn * pair, pair), pair)
                acc[...] += jnp.dot(
                    rows_p[kl, :, at], halves[kl, at, :], preferred_element_type=jnp.float32
                )
                return carry

            lax.fori_loop(0, lax.div(used[kl] + 1, 2), add, 0)
            for y in range(2):
                for z in range(n_z):
                    for c, ref in ((core, own_ref), (1 - core, other_ref)):
                        at = pl.multiple_of((z * 4 + y * 2 + c) * chunk, chunk)
                        ref[panel, y, z, kl] = acc[pl.ds(at, chunk), :].astype(ref.dtype)


def scatter_kernel(
    own, other, out_ref, sum_bf, fin_bf, from_core, from_y, from_z,
    send_sem, core_recv, y_recv, z_recv,
):
    panels, n_z = own.shape[0], own.shape[2]
    f32, bf16 = jnp.float32, jnp.bfloat16
    mine_g, mine = lax.axis_index("grp"), lax.axis_index("pq")
    core, yy, zz, nearest, _ = coords(mine)
    core_peer = (mine_g, pq_of(zz, yy, 1 - core))
    y_peer = (mine_g, pq_of(zz, 1 - yy, core))
    far_first = nearest[::-1] + (zz,)
    z_peers = [(mine_g, pq_of(z, yy, core)) for z in far_first[:-1]]
    meet([core_peer, y_peer] + z_peers)
    sent = []

    def push(src, dst, recv, peer):
        copy = pltpu.make_async_remote_copy(
            src_ref=src, dst_ref=dst, send_sem=send_sem.at[len(sent)],
            recv_sem=recv, device_id=peer, device_id_type=MESH,
        )
        copy.start()
        sent.append(copy)

    def landed(dst, recv):
        pltpu.make_async_copy(dst, dst, recv).wait()

    for y in (1 - yy, yy):
        for panel in range(panels):
            push(other.at[panel, y], from_core.at[panel, y], core_recv.at[panel, y], core_peer)
    for panel in range(panels):
        landed(from_core.at[panel, 1 - yy], core_recv.at[panel, 1 - yy])
    for s, z in enumerate(far_first):
        for panel in range(panels):
            total = own[panel, 1 - yy, z] + from_core[panel, 1 - yy, z].astype(f32)
            sum_bf[panel, s] = total.astype(bf16)
            push(sum_bf.at[panel, s], from_y.at[panel, s], y_recv.at[panel, s], y_peer)
    for panel in range(panels):
        landed(from_core.at[panel, yy], core_recv.at[panel, yy])
    for s, z in enumerate(far_first):
        for panel in range(panels):
            landed(from_y.at[panel, s], y_recv.at[panel, s])
            total = (
                own[panel, yy, z] + from_core[panel, yy, z].astype(f32)
                + from_y[panel, s].astype(f32)
            )
            if s < n_z - 1:
                fin_bf[panel, s] = total.astype(bf16)
                push(fin_bf.at[panel, s], from_z.at[panel, zz], z_recv.at[panel, zz], z_peers[s])
            else:
                out_ref[pl.ds(panel * KL_PANEL, KL_PANEL)] = total
    for panel in range(panels):
        total = out_ref[pl.ds(panel * KL_PANEL, KL_PANEL)]
        for z in nearest:
            landed(from_z.at[panel, z], z_recv.at[panel, z])
            total += from_z[panel, z].astype(f32)
        out_ref[pl.ds(panel * KL_PANEL, KL_PANEL)] = total
    for copy in sent:
        copy.wait_send()


def direct(n_grp, n_pq, pair_blocks, block_list, block_count, coef):
    panels, slots, tile, _ = pair_blocks.shape
    rows, cols = coef.shape
    width, nao, n_z = n_grp * cols, n_pq * rows, n_pq // 4
    chunk = width // n_pq
    bf16, f32 = jnp.bfloat16, jnp.float32
    vmem = pl.BlockSpec(memory_space=pltpu.VMEM)
    smem = pl.BlockSpec(memory_space=pltpu.SMEM)
    sems = pltpu.SemaphoreType.DMA
    shape = jax.ShapeDtypeStruct
    mib = 2**20
    subs = rows // tile
    n_gather = subs * (5 + 4 * (n_z - 1) + 4 * n_z)
    full, flipped = pl.pallas_call(
        functools.partial(gather_kernel, n_grp, n_pq, tile),
        out_shape=(shape((n_grp, nao, cols), bf16), shape((nao // tile, width, tile), bf16)),
        in_specs=[pl.BlockSpec(memory_space=pltpu.HBM)],
        out_specs=(vmem, vmem),
        scratch_shapes=[sems((n_gather,)), sems((n_grp, n_pq, subs)), sems],
        cost_estimate=pl.CostEstimate(
            flops=2 * nao * nao * width, bytes_accessed=8 * nao * width, transcendentals=0
        ),
        compiler_params=pltpu.CompilerParams(
            collective_id=0, has_side_effects=True, vmem_limit_bytes=24 * mib
        ),
    )(coef)
    padded = slots + 1 + slots % 2
    part = (panels, 2, n_z, KL_PANEL, chunk, width)
    own, other = pl.pallas_call(
        functools.partial(transform_kernel, n_grp, n_pq),
        out_shape=(shape(part, f32), shape(part, bf16)),
        in_specs=[vmem, smem, smem, vmem, vmem],
        out_specs=(vmem, vmem),
        scratch_shapes=[
            pltpu.VMEM((KL_PANEL + 1, width, padded * tile), bf16),
            pltpu.VMEM((KL_PANEL + 1, padded * tile, width), bf16),
            pltpu.VMEM((width, width), f32),
        ],
        compiler_params=pltpu.CompilerParams(vmem_limit_bytes=40 * mib),
    )(pair_blocks, block_list, block_count.reshape(panels), full, flipped)
    pieces = (panels, n_z, KL_PANEL, chunk, width)
    return pl.pallas_call(
        scatter_kernel,
        out_shape=shape((panels * KL_PANEL, chunk, width), f32),
        in_specs=[vmem, vmem],
        out_specs=vmem,
        scratch_shapes=[
            pltpu.VMEM(pieces, bf16),
            pltpu.VMEM(pieces, bf16),
            pltpu.VMEM(part, bf16),
            pltpu.VMEM(pieces, bf16),
            pltpu.VMEM(pieces, bf16),
            sems((panels * (1 + 2 * n_z) + panels,)),
            sems((panels, 2)),
            sems((panels, n_z)),
            sems((panels, n_z)),
        ],
        compiler_params=pltpu.CompilerParams(
            collective_id=1, has_side_effects=True, vmem_limit_bytes=24 * mib
        ),
    )(own, other)


def local_kernel(nblk, blocks_ref, list_ref, count_ref, coef_ref, out_ref):
    panels, slots, tile = blocks_ref.shape[0], blocks_ref.shape[1], blocks_ref.shape[2]
    out_ref[...] = jnp.zeros_like(out_ref)
    for panel in range(panels):

        def step(slot, carry):
            ident = list_ref[panel, slot]
            which = panel * KL_PANEL + lax.div(ident, nblk * nblk)
            row_blk = lax.rem(lax.div(ident, nblk), nblk)
            col_blk = lax.rem(ident, nblk)
            col_coef = coef_ref[pl.ds(pl.multiple_of(col_blk * tile, tile), tile), :]
            row_coef = coef_ref[pl.ds(pl.multiple_of(row_blk * tile, tile), tile), :]
            half = jnp.dot(blocks_ref[panel, slot], col_coef, preferred_element_type=jnp.float32)
            out_ref[which] += lax.dot_general(
                row_coef, half.astype(jnp.bfloat16), (((0,), (0,)), ((), ())),
                preferred_element_type=jnp.float32,
            )
            return carry

        lax.fori_loop(0, count_ref[panel, 0], step, 0)


def gathered(pair_blocks, block_list, block_count, coef):
    coef_rows = lax.all_gather(coef, "pq", axis=0, tiled=True)
    coef_full = lax.all_gather(coef_rows, "grp", axis=1, tiled=True)
    nao, width = coef_full.shape
    vmem = pl.BlockSpec(memory_space=pltpu.VMEM)
    smem = pl.BlockSpec(memory_space=pltpu.SMEM)
    joined = pl.pallas_call(
        functools.partial(local_kernel, nao // pair_blocks.shape[2]),
        out_shape=jax.ShapeDtypeStruct((pair_blocks.shape[0] * KL_PANEL, width, width), jnp.float32),
        in_specs=[vmem, smem, smem, vmem],
        out_specs=vmem,
        compiler_params=pltpu.CompilerParams(vmem_limit_bytes=48 * 2**20),
    )(pair_blocks, block_list, block_count, coef_full)
    return lax.psum_scatter(joined, "pq", scatter_dimension=1, tiled=True)


def body(pair_blocks, block_list, block_count, coef):
    n_grp, n_pq = lax.axis_size("grp"), lax.axis_size("pq")
    rows, cols = coef.shape
    tile = pair_blocks.shape[2]
    fits = n_grp == 2 and n_pq == 4 * LINE
    if fits and rows % tile == 0 and cols % 128 == 0:
        return direct(n_grp, n_pq, pair_blocks, block_list, block_count, coef)
    return gathered(pair_blocks, block_list, block_count, coef)


def solution(mesh):
    in_specs = (P("grp", "pq", None, None), P("grp", "pq"), P("grp", "pq"), P("pq", "grp"))
    out_specs = P("grp", "pq", None)
    return jax.shard_map(body, mesh=mesh, in_specs=in_specs, out_specs=out_specs, check_vma=False)
```

```python
import functools

import jax
import jax.numpy as jnp
from jax import lax
from jax.experimental import pallas as pl
from jax.experimental.pallas import tpu as pltpu
from jax.sharding import PartitionSpec as P

KL_PANEL = 2
MESH = pl.DeviceIdType.MESH
UNROLL = 6


LINE = 4


def coords(mine):
    core, yy, zz = lax.rem(mine, 2), lax.rem(lax.div(mine, 2), 2), lax.div(mine, 4)
    half = lax.div(zz, 2)
    beside = 2 * half + 1 - lax.rem(zz, 2)
    across = 3 - zz
    return core, yy, zz, (beside, 2 - half, 3 - 3 * half), across


def pq_of(z, y, c):
    return z * 4 + y * 2 + c


def meet(peers):
    barrier = pltpu.get_barrier_semaphore()
    for peer in peers:
        pl.semaphore_signal(barrier, inc=1, device_id=peer, device_id_type=MESH)
    pl.semaphore_wait(barrier, len(peers))


def gather_kernel(n_grp, n_pq, tile, coef_ref, full, flipped, send_sem, recv_sem, load_sem):
    rows, cols = coef_ref.shape
    subs = rows // tile
    mine_g, mine = lax.axis_index("grp"), lax.axis_index("pq")
    core, yy, zz, nearest, across = coords(mine)
    middle = (zz > 0) & (zz < LINE - 1)
    core_peer = (mine_g, pq_of(zz, yy, 1 - core))
    y_peer = (mine_g, pq_of(zz, 1 - yy, core))
    x_peer = (1 - mine_g, mine)
    beside_peer = (mine_g, pq_of(nearest[0], yy, core))
    across_peer = (mine_g, pq_of(across, yy, core))

    def place(g, p, k):
        at = pl.multiple_of(p * rows + k * tile, tile)
        return full.at[g, pl.ds(at, tile), :]

    own_rows = full.at[mine_g, pl.ds(pl.multiple_of(mine * rows, rows), rows), :]
    load = pltpu.make_async_copy(coef_ref, own_rows, load_sem)
    load.start()
    meet([core_peer, y_peer, x_peer, beside_peer, across_peer])
    load.wait()

    first_g, first_y = lax.rem(mine_g + 1 - core, 2), lax.rem(yy + core, 2)
    second_g, second_y = lax.rem(mine_g + core, 2), lax.rem(yy + 1 - core, 2)
    first_peer = (first_g, pq_of(zz, first_y, core))
    second_peer = (second_g, pq_of(zz, second_y, core))
    started = []

    def send(g, p, k, peer, only=None):
        copy = pltpu.make_async_remote_copy(
            src_ref=place(g, p, k), dst_ref=place(g, p, k), send_sem=send_sem.at[len(started)],
            recv_sem=recv_sem.at[g, p, k], device_id=peer, device_id_type=MESH,
        )
        if only is None:
            copy.start()
        else:
            pl.when(only)(copy.start)
        started.append((copy, only))

    def flip(g, p, k):
        at = pl.multiple_of(g * cols, cols)
        flipped[p * subs + k, pl.ds(at, cols), :] = place(g, p, k)[...].T

    def await_piece(g, p, k):
        pltpu.make_async_copy(place(g, p, k), place(g, p, k), recv_sem.at[g, p, k]).wait()

    z_of = (zz,) + nearest
    home = {
        "Z": (mine_g, yy), "F": (first_g, first_y),
        "S": (second_g, second_y), "D": (1 - mine_g, 1 - yy),
    }
    twin = {"Z": "Z", "F": "S", "S": "F", "D": "D"}

    def relay(kind, step):
        g, y = home[kind]
        p = pq_of(z_of[step], y, core)
        for k in range(subs):
            await_piece(g, p, k)
            if kind == "Z":
                send(g, p, k, across_peer if step == 1 else beside_peer, middle)
                send(g, p, k, first_peer)
            if kind in "ZF":
                send(g, p, k, second_peer)
            send(g, p, k, core_peer)
            flip(g, p, k)

    def take(kind, step):
        g, y = home[twin[kind]]
        p = pq_of(z_of[step], y, 1 - core)
        for k in range(subs):
            await_piece(g, p, k)
            flip(g, p, k)

    for k in range(subs):
        send(mine_g, mine, k, beside_peer)
        send(mine_g, mine, k, across_peer, middle)
        send(mine_g, mine, k, first_peer)
        send(mine_g, mine, k, second_peer)
    for k in range(subs):
        send(mine_g, mine, k, core_peer)
    for k in range(subs):
        flip(mine_g, mine, k)
    waves = ("Z1 F0", "Z2 F1", "S0 Z3 F2", "S1 D0 F3", "S2 D1", "S3 D2 D3")
    behind = ("", "Z0") + waves
    for turn, wave in enumerate(waves):
        for item in wave.split():
            relay(item[0], int(item[1]))
        for item in behind[turn].split():
            take(item[0], int(item[1]))
    for wave in behind[len(waves):]:
        for item in wave.split():
            take(item[0], int(item[1]))
    for copy, only in started:
        if only is None:
            copy.wait_send()
        else:
            pl.when(only)(copy.wait_send)


def transform_kernel(
    n_grp, n_pq, blocks_ref, list_ref, count_ref, full, flipped,
    own_ref, other_ref, rows_p, halves, acc,
):
    panels, slots, tile = blocks_ref.shape[0], blocks_ref.shape[1], blocks_ref.shape[2]
    nblk, width = flipped.shape[0], flipped.shape[1]
    cols, chunk, n_z = width // n_grp, width // n_pq, n_pq // 4
    core = lax.rem(lax.axis_index("pq"), 2)
    pair = 2 * tile

    for panel in range(panels):
        count = count_ref[panel]

        def step(turn, used):
            for k in range(UNROLL):
                slot = turn * UNROLL + k
                live = slot < count
                slot = jnp.minimum(slot, slots - 1)
                ident = list_ref[panel, slot]
                which = jnp.where(live, lax.div(ident, nblk * nblk), KL_PANEL)
                row_blk = lax.rem(lax.div(ident, nblk), nblk)
                col_blk = lax.rem(ident, nblk)
                spot = jnp.where(which == 0, used[0], jnp.where(which == 1, used[1], 0))
                used = tuple(u + jnp.where(which == kl, 1, 0) for kl, u in enumerate(used))
                at = pl.ds(pl.multiple_of(spot * tile, tile), tile)
                rows_p[which, :, at] = flipped[row_blk]
                for g in range(n_grp):
                    coefs = full[g, pl.ds(pl.multiple_of(col_blk * tile, tile), tile), :]
                    half = jnp.dot(blocks_ref[panel, slot], coefs, preferred_element_type=jnp.float32)
                    halves[which, at, g * cols:(g + 1) * cols] = half.astype(jnp.bfloat16)
            return used

        zero = jnp.int32(0)
        used = lax.fori_loop(0, lax.div(count + UNROLL - 1, UNROLL), step, (zero,) * KL_PANEL)
        for kl in range(KL_PANEL):
            at = pl.ds(pl.multiple_of(used[kl] * tile, tile), tile)
            rows_p[kl, :, at] = jnp.zeros((width, tile), jnp.bfloat16)
            halves[kl, at, :] = jnp.zeros((tile, width), jnp.bfloat16)
            acc[...] = jnp.zeros_like(acc)

            def add(turn, carry):
                at = pl.ds(pl.multiple_of(turn * pair, pair), pair)
                acc[...] += jnp.dot(
                    rows_p[kl, :, at], halves[kl, at, :], preferred_element_type=jnp.float32
                )
                return carry

            lax.fori_loop(0, lax.div(used[kl] + 1, 2), add, 0)
            for y in range(2):
                for z in range(n_z):
                    for c, ref in ((core, own_ref), (1 - core, other_ref)):
                        at = pl.multiple_of((z * 4 + y * 2 + c) * chunk, chunk)
                        ref[panel, y, z, kl] = acc[pl.ds(at, chunk), :].astype(ref.dtype)


def scatter_kernel(
    own, other, out_ref, sum_bf, fin_bf, from_core, from_y, from_z,
    send_sem, core_recv, y_recv, z_recv,
):
    panels, n_z = own.shape[0], own.shape[2]
    f32, bf16 = jnp.float32, jnp.bfloat16
    mine_g, mine = lax.axis_index("grp"), lax.axis_index("pq")
    core, yy, zz, nearest, _ = coords(mine)
    core_peer = (mine_g, pq_of(zz, yy, 1 - core))
    y_peer = (mine_g, pq_of(zz, 1 - yy, core))
    far_first = nearest[::-1] + (zz,)
    z_peers = [(mine_g, pq_of(z, yy, core)) for z in far_first[:-1]]
    meet([core_peer, y_peer] + z_peers)
    sent = []

    def push(src, dst, recv, peer):
        copy = pltpu.make_async_remote_copy(
            src_ref=src, dst_ref=dst, send_sem=send_sem.at[len(sent)],
            recv_sem=recv, device_id=peer, device_id_type=MESH,
        )
        copy.start()
        sent.append(copy)

    def landed(dst, recv):
        pltpu.make_async_copy(dst, dst, recv).wait()

    for y in (1 - yy, yy):
        for panel in range(panels):
            push(other.at[panel, y], from_core.at[panel, y], core_recv.at[panel, y], core_peer)
    for panel in range(panels):
        landed(from_core.at[panel, 1 - yy], core_recv.at[panel, 1 - yy])
    for s, z in enumerate(far_first):
        for panel in range(panels):
            total = own[panel, 1 - yy, z] + from_core[panel, 1 - yy, z].astype(f32)
            sum_bf[panel, s] = total.astype(bf16)
            push(sum_bf.at[panel, s], from_y.at[panel, s], y_recv.at[panel, s], y_peer)
    for panel in range(panels):
        landed(from_core.at[panel, yy], core_recv.at[panel, yy])
    for s, z in enumerate(far_first):
        for panel in range(panels):
            landed(from_y.at[panel, s], y_recv.at[panel, s])
            total = (
                own[panel, yy, z] + from_core[panel, yy, z].astype(f32)
                + from_y[panel, s].astype(f32)
            )
            if s < n_z - 1:
                fin_bf[panel, s] = total.astype(bf16)
                push(fin_bf.at[panel, s], from_z.at[panel, zz], z_recv.at[panel, zz], z_peers[s])
            else:
                out_ref[pl.ds(panel * KL_PANEL, KL_PANEL)] = total
    for panel in range(panels):
        total = out_ref[pl.ds(panel * KL_PANEL, KL_PANEL)]
        for z in nearest:
            landed(from_z.at[panel, z], z_recv.at[panel, z])
            total += from_z[panel, z].astype(f32)
        out_ref[pl.ds(panel * KL_PANEL, KL_PANEL)] = total
    for copy in sent:
        copy.wait_send()


def direct(n_grp, n_pq, pair_blocks, block_list, block_count, coef):
    panels, slots, tile, _ = pair_blocks.shape
    rows, cols = coef.shape
    width, nao, n_z = n_grp * cols, n_pq * rows, n_pq // 4
    chunk = width // n_pq
    bf16, f32 = jnp.bfloat16, jnp.float32
    vmem = pl.BlockSpec(memory_space=pltpu.VMEM)
    smem = pl.BlockSpec(memory_space=pltpu.SMEM)
    sems = pltpu.SemaphoreType.DMA
    shape = jax.ShapeDtypeStruct
    mib = 2**20
    subs = rows // tile
    n_gather = subs * (5 + 4 * (n_z - 1) + 4 * n_z)
    full, flipped = pl.pallas_call(
        functools.partial(gather_kernel, n_grp, n_pq, tile),
        out_shape=(shape((n_grp, nao, cols), bf16), shape((nao // tile, width, tile), bf16)),
        in_specs=[pl.BlockSpec(memory_space=pltpu.HBM)],
        out_specs=(vmem, vmem),
        scratch_shapes=[sems((n_gather,)), sems((n_grp, n_pq, subs)), sems],
        cost_estimate=pl.CostEstimate(
            flops=2 * nao * nao * width, bytes_accessed=8 * nao * width, transcendentals=0
        ),
        compiler_params=pltpu.CompilerParams(
            collective_id=0, has_side_effects=True, vmem_limit_bytes=24 * mib
        ),
    )(coef)
    padded = slots + 1 + slots % 2
    part = (panels, 2, n_z, KL_PANEL, chunk, width)
    own, other = pl.pallas_call(
        functools.partial(transform_kernel, n_grp, n_pq),
        out_shape=(shape(part, f32), shape(part, bf16)),
        in_specs=[vmem, smem, smem, vmem, vmem],
        out_specs=(vmem, vmem),
        scratch_shapes=[
            pltpu.VMEM((KL_PANEL + 1, width, padded * tile), bf16),
            pltpu.VMEM((KL_PANEL + 1, padded * tile, width), bf16),
            pltpu.VMEM((width, width), f32),
        ],
        compiler_params=pltpu.CompilerParams(vmem_limit_bytes=40 * mib),
    )(pair_blocks, block_list, block_count.reshape(panels), full, flipped)
    pieces = (panels, n_z, KL_PANEL, chunk, width)
    return pl.pallas_call(
        scatter_kernel,
        out_shape=shape((panels * KL_PANEL, chunk, width), f32),
        in_specs=[vmem, vmem],
        out_specs=vmem,
        scratch_shapes=[
            pltpu.VMEM(pieces, bf16),
            pltpu.VMEM(pieces, bf16),
            pltpu.VMEM(part, bf16),
            pltpu.VMEM(pieces, bf16),
            pltpu.VMEM(pieces, bf16),
            sems((panels * (1 + 2 * n_z) + panels,)),
            sems((panels, 2)),
            sems((panels, n_z)),
            sems((panels, n_z)),
        ],
        compiler_params=pltpu.CompilerParams(
            collective_id=1, has_side_effects=True, vmem_limit_bytes=24 * mib
        ),
    )(own, other)


def local_kernel(nblk, blocks_ref, list_ref, count_ref, coef_ref, out_ref):
    panels, slots, tile = blocks_ref.shape[0], blocks_ref.shape[1], blocks_ref.shape[2]
    out_ref[...] = jnp.zeros_like(out_ref)
    for panel in range(panels):

        def step(slot, carry):
            ident = list_ref[panel, slot]
            which = panel * KL_PANEL + lax.div(ident, nblk * nblk)
            row_blk = lax.rem(lax.div(ident, nblk), nblk)
            col_blk = lax.rem(ident, nblk)
            col_coef = coef_ref[pl.ds(pl.multiple_of(col_blk * tile, tile), tile), :]
            row_coef = coef_ref[pl.ds(pl.multiple_of(row_blk * tile, tile), tile), :]
            half = jnp.dot(blocks_ref[panel, slot], col_coef, preferred_element_type=jnp.float32)
            out_ref[which] += lax.dot_general(
                row_coef, half.astype(jnp.bfloat16), (((0,), (0,)), ((), ())),
                preferred_element_type=jnp.float32,
            )
            return carry

        lax.fori_loop(0, count_ref[panel, 0], step, 0)


def gathered(pair_blocks, block_list, block_count, coef):
    coef_rows = lax.all_gather(coef, "pq", axis=0, tiled=True)
    coef_full = lax.all_gather(coef_rows, "grp", axis=1, tiled=True)
    nao, width = coef_full.shape
    vmem = pl.BlockSpec(memory_space=pltpu.VMEM)
    smem = pl.BlockSpec(memory_space=pltpu.SMEM)
    joined = pl.pallas_call(
        functools.partial(local_kernel, nao // pair_blocks.shape[2]),
        out_shape=jax.ShapeDtypeStruct((pair_blocks.shape[0] * KL_PANEL, width, width), jnp.float32),
        in_specs=[vmem, smem, smem, vmem],
        out_specs=vmem,
        compiler_params=pltpu.CompilerParams(vmem_limit_bytes=48 * 2**20),
    )(pair_blocks, block_list, block_count, coef_full)
    return lax.psum_scatter(joined, "pq", scatter_dimension=1, tiled=True)


def body(pair_blocks, block_list, block_count, coef):
    n_grp, n_pq = lax.axis_size("grp"), lax.axis_size("pq")
    rows, cols = coef.shape
    tile = pair_blocks.shape[2]
    fits = n_grp == 2 and n_pq == 4 * LINE
    if fits and rows % tile == 0 and cols % 128 == 0:
        return direct(n_grp, n_pq, pair_blocks, block_list, block_count, coef)
    return gathered(pair_blocks, block_list, block_count, coef)


def solution(mesh):
    in_specs = (P("grp", "pq", None, None), P("grp", "pq"), P("grp", "pq"), P("pq", "grp"))
    out_specs = P("grp", "pq", None)
    return jax.shard_map(body, mesh=mesh, in_specs=in_specs, out_specs=out_specs, check_vma=False)
```
